512 devices in a mesh: row: 8 (over y, core), col: 16 (over z), depth: 4 (over x).
Axes of the slice: x: 4, y: 4, z: 16, core: 2. Of those that a mesh axis runs over, the one named last changes fastest.
Arguments:
- state_matrix: float32 [6144, 6144], P('row', 'col'), as said below
- gram_factor: float32 [6144, 256], P(('col', 'depth'), 'row'), as said below
Outputs:
- squared: float32 [6144, 6144], P('row', ('col', 'depth'))
- appended: float32 [6144, 256], P(('row', 'col', 'depth'))
- norm_ratio: float32 [256], replicated
Inputs may be any that keep to these rules, and one draw needn't show every extreme that they name: `gram_factor`: entries whose scale grows up to about ninefold along the rows; the columns differ in scale by up to tenfold. `state_matrix`: A real matrix with entries of order one on the diagonal and smaller ones elsewhere.
All inputs are finite; a program needn't handle non-finite values.
Results may differ from the reference program's by a relative error of at most 0.000073.
Values sent between devices are 32-bit elements; how exact they have to be, the bound alone decides.
A program may use at most 64 MiB of HBM per device.

```python
import math
import jax
import jax.numpy as jnp
from jax import lax

ORDER = 6144
RANK = 256


def draw_state_matrix(key, part):
    first, second, third = jax.random.split(jax.random.fold_in(key, 11), 3)
    noise = jax.random.normal(first, (ORDER, ORDER), jnp.float32)
    magnitude = jax.random.uniform(second, (ORDER,), jnp.float32, 0.1, 0.9)
    signs = jnp.where(jax.random.uniform(third, (ORDER,), jnp.float32) < 0.5, -1.0, 1.0)
    return noise * (0.6 / math.sqrt(ORDER)) + jnp.diag(signs * magnitude)


def draw_gram_factor(key, part):
    first, second, third = jax.random.split(jax.random.fold_in(key, 23), 3)
    positions = jnp.arange(ORDER, dtype=jnp.float32) / ORDER
    row_scale = jnp.exp(math.log(3.0) * positions + jax.random.uniform(second, (ORDER,), jnp.float32, 0.0, math.log(3.0)))
    col_scale = jnp.exp(jax.random.uniform(third, (RANK,), jnp.float32, math.log(0.3), math.log(3.0)))
    noise = jax.random.normal(first, (ORDER, RANK), jnp.float32)
    return noise * row_scale[:, None] * col_scale[None, :]


def setup_inputs(seed: int = 0) -> dict:
    streams_of = jax.random.split(jax.random.key(seed), 3)
    state_matrix = draw_state_matrix(jax.random.fold_in(streams_of[2], 71), 0)
    gram_factor = draw_gram_factor(jax.random.fold_in(streams_of[2], 71), 0)
    return {"state_matrix": state_matrix, "gram_factor": gram_factor}


def reference(state_matrix, gram_factor):
    squared = jnp.dot(state_matrix, state_matrix, preferred_element_type=jnp.float32, precision=lax.Precision.HIGHEST)
    appended = jnp.dot(state_matrix, gram_factor, preferred_element_type=jnp.float32, precision=lax.Precision.HIGHEST)
    new_sq = lax.optimization_barrier(jnp.sum(appended * appended, axis=0))
    old_sq = lax.optimization_barrier(jnp.sum(gram_factor * gram_factor, axis=0))
    norm_ratio = jnp.sqrt(new_sq) / jnp.sqrt(old_sq + 1e-06)
    return (squared, appended, norm_ratio)
```

```python
import functools

import jax
import jax.numpy as jnp
from jax import lax
from jax.experimental import pallas as pl
from jax.experimental.pallas import tpu as pltpu
from jax.sharding import PartitionSpec as P

MESH = pl.DeviceIdType.MESH
NR, NC, ND = 8, 16, 4
SUBS = 4
F32 = jnp.float32
BF16 = jnp.bfloat16
NT = (((1,), (1,)), ((), ()))
NN = (((1,), (0,)), ((), ()))


def split(v):
    hi = v.astype(BF16)
    return hi, (v - hi.astype(F32)).astype(BF16)


def product3(a, b, dims):
    a_hi, a_lo = split(a)
    b_hi, b_lo = split(b)
    dot = functools.partial(lax.dot_general, dimension_numbers=dims, preferred_element_type=F32)
    return dot(a_hi, b_hi) + (dot(a_hi, b_lo) + dot(a_lo, b_hi))


def kernel(
    a_hbm, g_hbm, sq_hbm, app_hbm, norm_hbm,
    zg, blk, zin, zall, pst, r1, s1, ra, rb, rd, sb, app, sx, sr, sz, nrm, acc, stage, cout,
    lsem, zsend, zrecv, bsend, brecv, gsend, grecv_x, grecv_r, psend, precv1, precv2,
    ssend, srecv_x, srecv_r, srecv_z, csend, crecv, osem,
):
    r, z, d = lax.axis_index("row"), lax.axis_index("col"), lax.axis_index("depth")
    rows, width = blk.shape[1], blk.shape[2]
    part = rows // ND
    sub = part // SUBS
    partner = r + 1 - 2 * (r % 2)
    pos, grp = z % 4, z // 4
    up, down = (z + 1) % NC, (z + NC - 1) % NC

    def at(i, size):
        return pl.ds(pl.multiple_of(i * size, 8), size)

    def remote(src, dst, send, recv, **device):
        return pltpu.make_async_remote_copy(
            src_ref=src, dst_ref=dst, send_sem=send, recv_sem=recv, device_id=device, device_id_type=MESH
        )

    started = []

    def go(copy):
        copy.start()
        started.append(copy)

    load_block = pltpu.make_async_copy(a_hbm, blk.at[r], lsem.at[0])
    load_own = pltpu.make_async_copy(a_hbm.at[at(d, part), :], zg.at[z], lsem.at[1])
    load_gram = pltpu.make_async_copy(g_hbm, zin, lsem.at[2])
    load_own.start()
    load_gram.start()
    load_block.start()

    barrier = pltpu.get_barrier_semaphore()
    peers = [{"col": (z + k) % NC} for k in (1, 15, 2, 14, 3, 13)]
    peers += [{"depth": (d + k) % ND} for k in range(1, ND)]
    peers += [{"row": (r + k) % NR} for k in range(1, NR)]
    for peer in peers:
        pl.semaphore_signal(barrier, inc=1, device_id=peer, device_id_type=MESH)
    load_gram.wait()
    zall[r, d] = zin[...].T
    pl.semaphore_wait(barrier, len(peers))

    def hop(way, k, s):
        source = (z - k + NC) % NC if way == 0 else (z + k) % NC
        piece = zg.at[source, pl.ds(s * sub, sub), :]
        return remote(piece, piece, zsend.at[way, k, s], zrecv.at[way, k, s], col=up if way == 0 else down)

    def travels(way, k, s):
        return k < 7 or (s < SUBS // 2) == (way == 0)

    def ring(k, subs=range(SUBS)):
        for s in subs:
            for way in (0, 1):
                if k > 0 and travels(way, k - 1, s):
                    hop(way, k - 1, s).wait_recv()
                if k < 8 and travels(way, k, s):
                    go(hop(way, k, s))

    n_sent = [0]

    def block_piece(b, q):
        return blk.at[b, at(q, part), :]

    def block_send(b, q, **device):
        go(remote(block_piece(b, q), block_piece(b, q), bsend.at[n_sent[0]], brecv.at[b, q], **device))
        n_sent[0] += 1

    def block_wait(b, q):
        remote(block_piece(b, q), block_piece(b, q), bsend.at[0], brecv.at[b, q], row=partner).wait_recv()

    q0, q1, q2, q3 = d, (d + 1) % ND, (d + 2) % ND, (d + 3) % ND
    above, below, across = (r + 2) % NR, (r + NR - 2) % NR, (r + 4) % NR
    right, left = (d + 1) % ND, (d + ND - 1) % ND

    def block_event_1():
        block_wait(below, q0)
        block_send(below, q0, row=above)
        block_send(below, q0, depth=right)
        block_send(below, q0, row=partner)
        block_wait(above, q1)
        block_send(above, q1, row=below)
        block_send(above, q1, depth=left)
        block_send(above, q1, row=partner)

    def block_event_2():
        block_wait(below, q1)
        block_send(below, q1, depth=left)
        block_send(below, q1, row=partner)
        block_wait(above, q0)
        block_send(above, q0, depth=right)
        block_send(above, q0, row=partner)
        block_wait(below, q3)
        block_send(below, q3, row=partner)
        block_wait(above, q2)
        block_send(above, q2, row=partner)

    def block_event_3():
        block_wait(across, q0)
        block_send(across, q0, depth=right)
        block_send(across, q0, row=partner)
        block_wait(across, q1)
        block_send(across, q1, depth=left)
        block_send(across, q1, row=partner)
        block_wait(above, q3)
        block_send(above, q3, row=partner)
        block_wait(below, q2)
        block_send(below, q2, row=partner)

    def block_event_4():
        block_wait(across, q3)
        block_send(across, q3, row=partner)
        block_wait(across, q2)
        block_send(across, q2, row=partner)
        for b in (partner, (partner + 2) % NR, (partner + 4) % NR, (partner + 6) % NR):
            for q in range(ND):
                block_wait(b, q)

    def chunk(source):
        left_op = zg[source]
        right_op = blk[source // 2, at(source % 2, width), :]
        acc[...] += product3(left_op, right_op, NN)

    def chunks(k):
        def one(i, _):
            chunk((z + NC + k - 2 * k * i) % NC)
            return 0

        lax.fori_loop(0, 2, one, 0)

    load_own.wait()
    ring(0)
    for k in range(1, ND):
        peer = (d + k) % ND
        go(remote(zall.at[r, d], zall.at[r, d], gsend.at[k], grecv_x.at[d], depth=peer))
    load_block.wait()
    block_send(r, q0, row=above)
    block_send(r, q1, row=below)
    block_send(r, q1, row=above)
    block_send(r, q0, row=below)
    for q in range(ND):
        block_send(r, q, row=partner)

    for k in range(1, ND):
        peer = (d + k) % ND
        remote(zall.at[r, peer], zall.at[r, peer], gsend.at[0], grecv_x.at[peer], depth=peer).wait_recv()
    for k in range(1, NR):
        peer = (r + k) % NR
        go(remote(zall.at[r], zall.at[r], gsend.at[3 + k], grecv_r.at[r], row=peer))
    for k in range(1, NR):
        peer = (r + k) % NR
        remote(zall.at[peer], zall.at[peer], gsend.at[0], grecv_r.at[peer], row=peer).wait_recv()
    rank = NR * zin.shape[1]
    factor = jnp.concatenate([zall[:, x].reshape(rank, zin.shape[0]) for x in range(ND)], axis=1)
    own_rows = app.shape[0]
    for b in range(ND):
        partial = product3(blk[r, pl.ds(b * part, part), :], factor, NT)
        for i in range(part // own_rows):
            pst[i % ND, i // ND, b] = partial[i * own_rows : (i + 1) * own_rows]
    squares = factor * factor
    s_hi, s_lo = split(squares)
    ones = jnp.ones((8, width), BF16)
    old = lax.dot_general(ones, s_hi, NT, preferred_element_type=F32) + lax.dot_general(
        ones, s_lo, NT, preferred_element_type=F32
    )
    sx[d, 2] = old[0, :128]
    sx[d, 3] = old[0, 128:]
    for k in range(1, 4):
        q = (pos + k) % 4
        go(remote(pst.at[d, q], r1.at[pos], psend.at[k], precv1.at[pos], col=grp * 4 + q))

    ring(1)
    block_event_1()
    ring(2)
    block_event_2()
    total = pst[d, pos]
    for k in range(1, 4):
        q = (pos + k) % 4
        remote(r1.at[q], r1.at[q], psend.at[0], precv1.at[q], col=up).wait_recv()
        total = total + r1[q]
    s1[...] = total
    far_up, far_down = (z + 4) % NC, (z + NC - 4) % NC
    go(remote(s1.at[(grp + 2) % 4], ra, psend.at[4], precv2.at[0], col=far_down))
    go(remote(s1.at[(grp + 1) % 4], rd, psend.at[5], precv2.at[1], col=far_up))
    ring(3)
    block_event_3()
    remote(ra, ra, psend.at[0], precv2.at[0], col=up).wait_recv()
    sb[...] = ra[...] + s1[(grp + 3) % 4]
    go(remote(sb, rb, psend.at[6], precv2.at[2], col=far_down))
    acc[...] = jnp.zeros_like(acc)
    ring(4)
    block_event_4()
    chunk(z)
    chunks(1)
    remote(rd, rd, psend.at[0], precv2.at[1], col=up).wait_recv()
    remote(rb, rb, psend.at[0], precv2.at[2], col=up).wait_recv()
    new = s1[grp] + rd[...] + rb[...]
    app[...] = new
    new_sq = jnp.sum(new * new, axis=0, keepdims=True)
    sx[d, 0] = new_sq[0, :128]
    sx[d, 1] = new_sq[0, 128:]
    store_app = pltpu.make_async_copy(app, app_hbm, osem.at[0])
    store_app.start()
    for k in range(1, ND):
        go(remote(sx.at[d], sx.at[d], ssend.at[k], srecv_x.at[d], depth=(d + k) % ND))
    ring(5, range(2))
    chunks(2)
    ring(5, range(2, SUBS))
    chunks(3)
    for k in range(1, ND):
        q = (d + k) % ND
        remote(sx.at[q], sx.at[q], ssend.at[0], srecv_x.at[q], depth=q).wait_recv()
    sr[r] = jnp.sum(sx[...], axis=0)
    for k in range(1, NR):
        go(remote(sr.at[r], sr.at[r], ssend.at[3 + k], srecv_r.at[r], row=(r + k) % NR))
    ring(6, range(2))
    chunks(4)
    for k in range(1, NR):
        q = (r + k) % NR
        remote(sr.at[q], sr.at[q], ssend.at[0], srecv_r.at[q], row=q).wait_recv()
    sz[z] = jnp.sum(sr[...], axis=0)
    for k in range(1, NC):
        go(remote(sz.at[z], sz.at[z], ssend.at[10 + k], srecv_z.at[z], col=(z + k) % NC))
    ring(6, range(2, SUBS))
    chunks(5)
    ring(7, range(2))
    chunks(6)
    ring(7, range(2, SUBS))
    chunks(7)
    ring(8)
    chunk((z + 8) % NC)

    wide = cout.shape[2]
    for x in range(ND):
        stage[x] = acc[:, x * wide : (x + 1) * wide]
    for k in range(1, ND):
        q = (d + k) % ND
        go(remote(stage.at[q], cout.at[d], csend.at[k], crecv.at[d], depth=q))
    store_own = pltpu.make_async_copy(stage.at[d], sq_hbm.at[at(d, part), :], osem.at[1])
    store_own.start()

    for k in range(1, NC):
        q = (z + k) % NC
        remote(sz.at[q], sz.at[q], ssend.at[0], srecv_z.at[q], col=q).wait_recv()
    sums = jnp.sum(sz[...], axis=0)
    nrm[...] = jnp.sqrt(sums[0:2]) / jnp.sqrt(sums[2:4] * (1.0 / (NR * ND)) + 1e-06)
    store_norm = pltpu.make_async_copy(nrm, norm_hbm, osem.at[2])
    store_norm.start()
    stores = [store_app, store_own, store_norm]
    for k in range(1, ND):
        q = (d + k) % ND
        remote(cout.at[q], cout.at[q], csend.at[0], crecv.at[q], depth=q).wait_recv()
        store = pltpu.make_async_copy(cout.at[q], sq_hbm.at[at(q, part), :], osem.at[2 + k])
        store.start()
        stores.append(store)
    for copy in started:
        copy.wait_send()
    for store in stores:
        store.wait()


def body(state_matrix, gram_factor):
    rows, width = state_matrix.shape
    factor_rows, factor_cols = gram_factor.shape
    part = rows // ND
    rank = factor_cols * NR
    wide = width // ND
    own_rows = rows // (NC * ND)
    dma = pltpu.SemaphoreType.DMA
    vmem = lambda *shape: pltpu.VMEM(shape, F32)
    squared, appended, norm = pl.pallas_call(
        kernel,
        out_shape=(
            jax.ShapeDtypeStruct((rows, wide), F32),
            jax.ShapeDtypeStruct((own_rows, rank), F32),
            jax.ShapeDtypeStruct((2, rank // 2), F32),
        ),
        in_specs=[pl.BlockSpec(memory_space=pl.ANY)] * 2,
        out_specs=[pl.BlockSpec(memory_space=pl.ANY)] * 3,
        scratch_shapes=[
            vmem(NC, part, width),
            vmem(NR, rows, width),
            vmem(factor_rows, factor_cols),
            vmem(NR, ND, factor_cols, factor_rows),
            vmem(ND, 4, 4, own_rows, rank),
            vmem(4, 4, own_rows, rank),
            vmem(4, own_rows, rank),
            vmem(own_rows, rank),
            vmem(own_rows, rank),
            vmem(own_rows, rank),
            vmem(own_rows, rank),
            vmem(own_rows, rank),
            vmem(ND, 4, 128),
            vmem(NR, 4, 128),
            vmem(NC, 4, 128),
            vmem(2, 128),
            vmem(part, width),
            vmem(ND, part, wide),
            vmem(ND, part, wide),
            dma((3,)),
            dma((2, 8, SUBS)),
            dma((2, 8, SUBS)),
            dma((40,)),
            dma((NR, ND)),
            dma((12,)),
            dma((ND,)),
            dma((NR,)),
            dma((8,)),
            dma((4,)),
            dma((3,)),
            dma((26,)),
            dma((ND,)),
            dma((NR,)),
            dma((NC,)),
            dma((ND,)),
            dma((ND,)),
            dma((6,)),
        ],
        compiler_params=pltpu.CompilerParams(
            collective_id=0, has_side_effects=True, vmem_limit_bytes=60 * 1024 * 1024
        ),
    )(state_matrix, gram_factor)
    return squared, appended, norm.reshape(rank)


def solution(mesh):
    in_specs = (P("row", "col"), P(("col", "depth"), "row"))
    out_specs = (P("row", ("col", "depth")), P(("row", "col", "depth"), None), P())
    return jax.shard_map(body, mesh=mesh, in_specs=in_specs, out_specs=out_specs, check_vma=False)
```

```python
import functools

import jax
import jax.numpy as jnp
from jax import lax
from jax.experimental import pallas as pl
from jax.experimental.pallas import tpu as pltpu
from jax.sharding import PartitionSpec as P

MESH = pl.DeviceIdType.MESH
NR, NC, ND = 8, 16, 4
SUBS = 6
EARLY = range(4)
LATE = range(4, 6)
LANES = 128
F32 = jnp.float32
BF16 = jnp.bfloat16
NT = (((1,), (1,)), ((), ()))
NN = (((1,), (0,)), ((), ()))


def split(v):
    hi = v.astype(BF16)
    return hi, (v - hi.astype(F32)).astype(BF16)


def product3(a, b, dims):
    a_hi, a_lo = split(a)
    b_hi, b_lo = split(b)
    dot = functools.partial(lax.dot_general, dimension_numbers=dims, preferred_element_type=F32)
    return dot(a_hi, b_hi) + (dot(a_hi, b_lo) + dot(a_lo, b_hi))


def kernel(
    a_hbm, g_hbm, cout_e, cout_l, app, nrm,
    zg, blk, zall, pst, r1, s1, r2, sx, sr, plane, sz, both, acc, stage_e, stage_l,
    lsem, zsend, zrecv, bsend, brecv, gsend, grecv_x, grecv_r, psend, precv1, precv2,
    ssend, srecv_x, srecv_r, srecv_z, srecv_c, csend, crecv_e, crecv_l, token,
):
    r, z, d = lax.axis_index("row"), lax.axis_index("col"), lax.axis_index("depth")
    rows, width = blk.shape[1], blk.shape[2]
    part = rows // ND
    sub = part // SUBS
    first = sub * len(EARLY)
    core = r % 2
    partner = r + 1 - 2 * core
    pos, grp = z % 4, z // 4
    up, down = (z + 1) % NC, (z + NC - 1) % NC
    above, below, across = (r + 2) % NR, (r + NR - 2) % NR, (r + 4) % NR
    right, left = (d + 1) % ND, (d + ND - 1) % ND

    def at(i, size):
        return pl.ds(pl.multiple_of(i * size, 8), size)

    def remote(src, dst, send, recv, **device):
        return pltpu.make_async_remote_copy(
            src_ref=src, dst_ref=dst, send_sem=send, recv_sem=recv, device_id=device, device_id_type=MESH
        )

    started = []

    def go(copy):
        copy.start()
        started.append(copy)

    def arrived(ref, recv):
        remote(ref, ref, csend.at[0], recv, row=partner).wait_recv()

    load_own = pltpu.make_async_copy(a_hbm.at[at(d, part), :], zg.at[z], lsem.at[0])
    load_gram = pltpu.make_async_copy(g_hbm, zall.at[r, d], lsem.at[1])
    load_block = pltpu.make_async_copy(a_hbm, blk.at[r], lsem.at[2])
    load_own.start()
    load_gram.start()
    load_block.start()

    barrier = pltpu.get_barrier_semaphore()
    peers = [{"col": (z + k) % NC} for k in (1, 15, 2, 14, 3, 13)]
    peers += [{"depth": (d + k) % ND} for k in range(1, ND)]
    peers += [{"row": (r + k) % NR} for k in range(1, NR)]
    for peer in peers:
        pl.semaphore_signal(barrier, inc=1, device_id=peer, device_id_type=MESH)
    acc[...] = jnp.zeros_like(acc)
    load_own.wait()
    load_gram.wait()
    load_block.wait()
    pl.semaphore_wait(barrier, len(peers))

    def piece(way, k, s):
        source = (z - k + NC) % NC if way == 0 else (z + k) % NC
        return zg.at[source, pl.ds(s * sub, sub), :]

    def travels(way, k, s):
        return k < 7 or s % 2 == way

    def ring(k, subs):
        for s in subs:
            for way in (0, 1):
                if k > 0 and travels(way, k - 1, s):
                    arrived(piece(way, k, s), zrecv.at[way, k - 1, s])
                if k < 8 and travels(way, k, s):
                    ref = piece(way, k, s)
                    go(remote(ref, ref, zsend.at[way, k, s], zrecv.at[way, k, s], col=up if way == 0 else down))

    n_sent = [0]

    def block_piece(b, q):
        return blk.at[b, at(q, part), :]

    def block_send(b, q, **device):
        go(remote(block_piece(b, q), block_piece(b, q), bsend.at[n_sent[0]], brecv.at[b, q], **device))
        n_sent[0] += 1

    def block_wait(b, q):
        arrived(block_piece(b, q), brecv.at[b, q])

    q0, q1, q2, q3 = d, (d + 1) % ND, (d + 2) % ND, (d + 3) % ND

    def block_event_1():
        block_wait(below, q0)
        block_send(below, q0, row=above)
        block_send(below, q0, depth=right)
        block_send(below, q0, row=partner)
        block_wait(above, q1)
        block_send(above, q1, row=below)
        block_send(above, q1, depth=left)
        block_send(above, q1, row=partner)

    def block_event_2():
        block_wait(below, q1)
        block_send(below, q1, depth=left)
        block_send(below, q1, row=partner)
        block_wait(above, q0)
        block_send(above, q0, depth=right)
        block_send(above, q0, row=partner)
        block_wait(below, q3)
        block_send(below, q3, row=partner)
        block_wait(above, q2)
        block_send(above, q2, row=partner)

    def block_event_3():
        block_wait(across, q0)
        block_send(across, q0, depth=right)
        block_send(across, q0, row=partner)
        block_wait(across, q1)
        block_send(across, q1, depth=left)
        block_send(across, q1, row=partner)
        block_wait(above, q3)
        block_send(above, q3, row=partner)
        block_wait(below, q2)
        block_send(below, q2, row=partner)

    def block_event_4():
        block_wait(across, q3)
        block_send(across, q3, row=partner)
        block_wait(across, q2)
        block_send(across, q2, row=partner)
        for b in (partner, (partner + 2) % NR, (partner + 4) % NR, (partner + 6) % NR):
            for q in range(ND):
                block_wait(b, q)

    def chunk(source, lo, hi):
        left_op = zg[source, lo:hi]
        right_op = blk[source // 2, at(source % 2, width), :]
        acc[lo:hi] += product3(left_op, right_op, NN)

    def chunks(k, lo=0, hi=part):
        def one(i, _):
            chunk((z + NC + k - 2 * k * i) % NC, lo, hi)
            return 0

        lax.fori_loop(0, 2, one, 0)

    ring(0, EARLY)
    for k in range(1, ND):
        go(remote(zall.at[r, d], zall.at[r, d], gsend.at[k], grecv_x.at[d], depth=(d + k) % ND))
    ring(0, LATE)
    for k in range(1, ND):
        q = (d + k) % ND
        arrived(zall.at[r, q], grecv_x.at[q])
    for k, peer in enumerate((above, below, across, partner)):
        go(remote(zall.at[r], zall.at[r], gsend.at[4 + k], grecv_r.at[r], row=peer))
    block_send(r, q0, row=above)
    block_send(r, q1, row=below)
    block_send(r, q1, row=above)
    block_send(r, q0, row=below)
    for q in range(ND):
        block_send(r, q, row=partner)

    ring(1, EARLY)
    ring(1, LATE)
    for k, peer in enumerate((above, below, across)):
        arrived(zall.at[peer], grecv_r.at[peer])
        go(remote(zall.at[peer], zall.at[peer], gsend.at[8 + k], grecv_r.at[peer], row=partner))
    ring(2, EARLY)
    far = [(z + 5) % NC, (z + NC - 5) % NC]
    for peer in far:
        pl.semaphore_signal(token, inc=1, device_id={"col": peer}, device_id_type=MESH)

    for peer in (partner, (partner + 2) % NR, (partner + 4) % NR, (partner + 6) % NR):
        arrived(zall.at[peer], grecv_r.at[peer])
    rank = NR * zall.shape[2]
    factor = jnp.concatenate([zall[:, x].reshape(rank, zall.shape[3]) for x in range(ND)], axis=1)
    own = app.shape[0]
    for b in range(ND):
        partial = product3(blk[r, pl.ds(b * part, part), :], factor, NT)
        for i in range(part // own):
            value = partial[i * own : (i + 1) * own]
            pst[i % ND, i // ND, b, 0:own] = value[:, :LANES]
            pst[i % ND, i // ND, b, own : 2 * own] = value[:, LANES:]
    s_hi, s_lo = split(factor * factor)
    ones = jnp.ones((8, width), BF16)
    old = lax.dot_general(ones, s_hi, NT, preferred_element_type=F32) + lax.dot_general(
        ones, s_lo, NT, preferred_element_type=F32
    )
    sx[d, 2] = old[0, :LANES]
    sx[d, 3] = old[0, LANES:]
    for k in range(1, 4):
        q = (pos + k) % 4
        go(remote(pst.at[d, q], r1.at[pos], psend.at[k - 1], precv1.at[pos], col=grp * 4 + q))

    ring(2, LATE)
    block_event_1()
    ring(3, EARLY)
    ring(3, LATE)
    block_event_2()
    total = pst[d, pos]
    for k in range(1, 4):
        q = (pos + k) % 4
        arrived(r1.at[q], precv1.at[q])
        total = total + r1[q]
    s1[...] = total
    pl.semaphore_wait(token, 2)
    for k in range(1, 4):
        q = (grp + k) % 4
        go(remote(s1.at[q], r2.at[grp], psend.at[2 + k], precv2.at[grp], col=q * 4 + pos))
    ring(4, EARLY)
    ring(5, EARLY)
    ring(4, LATE)
    block_event_3()
    ring(6, EARLY)
    new = s1[grp]
    for k in range(1, 4):
        q = (grp + k) % 4
        arrived(r2.at[q], precv2.at[q])
        new = new + r2[q]
    app[:, :LANES] = new[:own]
    app[:, LANES:] = new[own:]
    squares = new * new
    sx[d, 0] = jnp.sum(squares[:own], axis=0)
    sx[d, 1] = jnp.sum(squares[own:], axis=0)
    for k in range(1, ND):
        go(remote(sx.at[d], sx.at[d], ssend.at[k], srecv_x.at[d], depth=(d + k) % ND))
    block_event_4()
    chunk(z, 0, part)
    chunks(1)
    ring(5, LATE)
    for k in range(1, ND):
        q = (d + k) % ND
        arrived(sx.at[q], srecv_x.at[q])
    sr[r] = jnp.sum(sx[...], axis=0)
    for k in range(1, NR):
        go(remote(sr.at[r], sr.at[r], ssend.at[3 + k], srecv_r.at[r], row=(r + k) % NR))
    chunks(2)
    chunks(3)
    ring(7, EARLY)
    for k in range(1, NR):
        q = (r + k) % NR
        arrived(sr.at[q], srecv_r.at[q])
    sums = jnp.sum(sr[...], axis=0)
    plane[0] = sums[0:2]
    plane[1] = sums[2:4]
    sz[z] = plane[core]
    for k in range(1, NC):
        go(remote(sz.at[z], sz.at[z], ssend.at[10 + k], srecv_z.at[z], col=(z + k) % NC))
    chunks(4)
    chunks(5)
    ring(6, LATE)
    chunks(6)
    chunks(7, 0, first)
    ring(8, EARLY)
    chunk((z + 8) % NC, 0, first)

    wide = width // ND
    turned = acc[0:first].T
    for x in range(ND):
        stage_e[x] = turned[x * wide : (x + 1) * wide]
    for k in (2, 1, 3):
        q = (d + k) % ND
        go(remote(stage_e.at[q], cout_e.at[d], csend.at[k], crecv_e.at[d], depth=q))
    cout_e[d] = stage_e[d]
    ring(7, LATE)
    chunks(7, first, part)
    ring(8, LATE)
    chunk((z + 8) % NC, first, part)
    turned = acc[first:part].T
    for x in range(ND):
        block = turned[x * wide : (x + 1) * wide]
        stage_l[x] = jnp.concatenate([block[: wide // 2], block[wide // 2 :]], axis=1)
    for k in (2, 1, 3):
        q = (d + k) % ND
        go(remote(stage_l.at[q], cout_l.at[d], csend.at[3 + k], crecv_l.at[d], depth=q))
    cout_l[d] = stage_l[d]

    for k in range(1, NC):
        q = (z + k) % NC
        arrived(sz.at[q], srecv_z.at[q])
    both[core] = jnp.sum(sz[...], axis=0)
    go(remote(both.at[core], both.at[core], ssend.at[26], srecv_c, row=partner))
    for copy in started:
        copy.wait_send()
    arrived(both.at[1 - core], srecv_c)
    nrm[...] = jnp.sqrt(both[0]) / jnp.sqrt(both[1] * (1.0 / (NR * ND)) + 1e-06)
    for k in range(1, ND):
        q = (d + k) % ND
        arrived(cout_e.at[q], crecv_e.at[q])
        arrived(cout_l.at[q], crecv_l.at[q])


def finish(early, late, app_in, nrm_in, sq, app, nrm):
    half = early.shape[1] // 2
    app[...] = app_in[...]
    nrm[...] = nrm_in[...]
    for i in range(0, ND, 2):
        e0, e1 = early[i], early[i + 1]
        l0, l1 = late[i], late[i + 1]
        base = i * 3 * LANES // 2
        sq[:, base : base + LANES] = e0
        l0_cols = jnp.concatenate([l0[:, :64], l0[:, 64:]], axis=0)
        l1_cols = jnp.concatenate([l1[:, :64], l1[:, 64:]], axis=0)
        sq[:, base + LANES : base + 2 * LANES] = jnp.concatenate([l0_cols, e1[:, :64]], axis=1)
        sq[:, base + 2 * LANES : base + 3 * LANES] = jnp.concatenate([e1[:, 64:], l1_cols], axis=1)


def body(state_matrix, gram_factor):
    rows, width = state_matrix.shape
    factor_rows, factor_cols = gram_factor.shape
    part = rows // ND
    rank = factor_cols * NR
    wide = width // ND
    own = rows // (NC * ND)
    dma = pltpu.SemaphoreType.DMA
    vmem = lambda *shape: pltpu.VMEM(shape, F32)
    shape = lambda *dims: jax.ShapeDtypeStruct(dims, F32)
    whole = pl.BlockSpec(memory_space=pltpu.VMEM)
    parts = pl.pallas_call(
        kernel,
        out_shape=(shape(ND, wide, LANES), shape(ND, wide // 2, LANES), shape(own, rank), shape(2, LANES)),
        in_specs=[pl.BlockSpec(memory_space=pltpu.HBM)] * 2,
        out_specs=[whole] * 4,
        scratch_shapes=[
            vmem(NC, part, width),
            vmem(NR, rows, width),
            vmem(NR, ND, factor_cols, factor_rows),
            vmem(ND, 4, 4, 2 * own, LANES),
            vmem(4, 4, 2 * own, LANES),
            vmem(4, 2 * own, LANES),
            vmem(4, 2 * own, LANES),
            vmem(ND, 4, LANES),
            vmem(NR, 4, LANES),
            vmem(2, 2, LANES),
            vmem(NC, 2, LANES),
            vmem(2, 2, LANES),
            vmem(part, width),
            vmem(ND, wide, LANES),
            vmem(ND, wide // 2, LANES),
            dma((3,)),
            dma((2, 8, SUBS)),
            dma((2, 8, SUBS)),
            dma((40,)),
            dma((NR, ND)),
            dma((12,)),
            dma((ND,)),
            dma((NR,)),
            dma((8,)),
            dma((4,)),
            dma((4,)),
            dma((28,)),
            dma((ND,)),
            dma((NR,)),
            dma((NC,)),
            dma,
            dma((8,)),
            dma((ND,)),
            dma((ND,)),
            pltpu.SemaphoreType.REGULAR,
        ],
        compiler_params=pltpu.CompilerParams(
            collective_id=0, has_side_effects=True, vmem_limit_bytes=55900000
        ),
    )(state_matrix, gram_factor.T)
    squared, appended, norm = pl.pallas_call(
        finish,
        out_shape=(shape(wide, rows), shape(own, rank), shape(2, LANES)),
        in_specs=[whole] * 4,
        out_specs=[whole] * 3,
        compiler_params=pltpu.CompilerParams(vmem_limit_bytes=8 * 1024 * 1024),
    )(*parts)
    return squared.T, appended, norm.reshape(rank)


def solution(mesh):
    in_specs = (P("row", "col"), P(("col", "depth"), "row"))
    out_specs = (P("row", ("col", "depth")), P(("row", "col", "depth"), None), P())
    return jax.shard_map(body, mesh=mesh, in_specs=in_specs, out_specs=out_specs, check_vma=False)
```

```python
import functools

import jax
import jax.numpy as jnp
from jax import lax
from jax.experimental import pallas as pl
from jax.experimental.pallas import tpu as pltpu
from jax.sharding import PartitionSpec as P

MESH = pl.DeviceIdType.MESH
NR, NC, ND = 8, 16, 4
SUBS = 6
EARLY = range(4)
LATE = range(4, 6)
LANES = 128
F32 = jnp.float32
BF16 = jnp.bfloat16
NT = (((1,), (1,)), ((), ()))
NN = (((1,), (0,)), ((), ()))


def split(v):
    hi = v.astype(BF16)
    return hi, (v - hi.astype(F32)).astype(BF16)


def product3(a, b, dims):
    a_hi, a_lo = split(a)
    b_hi, b_lo = split(b)
    dot = functools.partial(lax.dot_general, dimension_numbers=dims, preferred_element_type=F32)
    return dot(a_hi, b_hi) + (dot(a_hi, b_lo) + dot(a_lo, b_hi))


def kernel(
    a_hbm, g_hbm, cout_e, cout_l, app, nrm,
    zg, blk, zall, pst, r1, s1, r2, sx, plane, sz, both, acc, stage_e, stage_l,
    lsem, zsend, zrecv, bsend, brecv, gsend, grecv_x, grecv_r, psend, precv1, precv2,
    ssend, srecv_x, srecv_z, srecv_c, csend, crecv_e, crecv_l, token_2, token_4,
):
    r, z, d = lax.axis_index("row"), lax.axis_index("col"), lax.axis_index("depth")
    rows, width = blk.shape[1], blk.shape[2]
    part = rows // ND
    sub = part // SUBS
    first = sub * len(EARLY)
    core = r % 2
    partner = r + 1 - 2 * core
    pos, grp = z % 4, z // 4
    here = r * ND + d
    up, down = (z + 1) % NC, (z + NC - 1) % NC
    above, below, across = (r + 2) % NR, (r + NR - 2) % NR, (r + 4) % NR
    right, left = (d + 1) % ND, (d + ND - 1) % ND

    def at(i, size):
        return pl.ds(pl.multiple_of(i * size, 8), size)

    def remote(src, dst, send, recv, **device):
        return pltpu.make_async_remote_copy(
            src_ref=src, dst_ref=dst, send_sem=send, recv_sem=recv, device_id=device, device_id_type=MESH
        )

    started = []

    def go(copy):
        copy.start()
        started.append(copy)

    def drain(left=0):
        while len(started) > left:
            started.pop(0).wait_send()

    def tell(token, distance):
        for peer in ((z + distance) % NC, (z + NC - distance) % NC):
            pl.semaphore_signal(token, inc=1, device_id={"col": peer}, device_id_type=MESH)

    def arrived(ref, recv):
        remote(ref, ref, csend.at[0], recv, row=partner).wait_recv()

    load_own = pltpu.make_async_copy(a_hbm.at[at(d, part), :], zg.at[z], lsem.at[0])
    load_gram = pltpu.make_async_copy(g_hbm, zall.at[r, d], lsem.at[1])
    load_block = pltpu.make_async_copy(a_hbm, blk.at[r], lsem.at[2])
    load_own.start()
    load_gram.start()
    load_block.start()

    barrier = pltpu.get_barrier_semaphore()
    peers = [{"col": up}, {"col": down}]
    peers += [{"depth": (d + k) % ND} for k in range(1, ND)]
    peers += [{"row": above}, {"row": below}, {"row": across}, {"row": partner}]
    for peer in peers:
        pl.semaphore_signal(barrier, inc=1, device_id=peer, device_id_type=MESH)
    acc[...] = jnp.zeros_like(acc)
    load_own.wait()
    load_gram.wait()
    load_block.wait()
    pl.semaphore_wait(barrier, len(peers))

    def piece(way, k, s):
        source = (z - k + NC) % NC if way == 0 else (z + k) % NC
        return zg.at[source, pl.ds(s * sub, sub), :]

    def travels(way, k, s):
        return k < 7 or s % 2 == way

    def ring(k, subs):
        for s in subs:
            for way in (0, 1):
                if k > 0 and travels(way, k - 1, s):
                    arrived(piece(way, k, s), zrecv.at[way, k - 1, s])
                if k < 8 and travels(way, k, s):
                    ref = piece(way, k, s)
                    go(remote(ref, ref, zsend.at[way, k, s], zrecv.at[way, k, s], col=up if way == 0 else down))

    n_sent = [0]

    def block_piece(b, q):
        return blk.at[b, at(q, part), :]

    def block_send(b, q, **device):
        go(remote(block_piece(b, q), block_piece(b, q), bsend.at[n_sent[0]], brecv.at[b, q], **device))
        n_sent[0] += 1

    def block_wait(b, q):
        arrived(block_piece(b, q), brecv.at[b, q])

    q0, q1, q2, q3 = d, (d + 1) % ND, (d + 2) % ND, (d + 3) % ND

    def block_event_1():
        block_wait(below, q0)
        block_send(below, q0, row=above)
        block_send(below, q0, depth=right)
        block_send(below, q0, row=partner)
        block_wait(above, q1)
        block_send(above, q1, row=below)
        block_send(above, q1, depth=left)
        block_send(above, q1, row=partner)

    def block_event_2():
        block_wait(below, q1)
        block_send(below, q1, depth=left)
        block_send(below, q1, row=partner)
        block_wait(above, q0)
        block_send(above, q0, depth=right)
        block_send(above, q0, row=partner)
        block_wait(below, q3)
        block_send(below, q3, row=partner)
        block_wait(above, q2)
        block_send(above, q2, row=partner)

    def block_event_3():
        block_wait(across, q0)
        block_send(across, q0, depth=right)
        block_send(across, q0, row=partner)
        block_wait(across, q1)
        block_send(across, q1, depth=left)
        block_send(across, q1, row=partner)
        block_wait(above, q3)
        block_send(above, q3, row=partner)
        block_wait(below, q2)
        block_send(below, q2, row=partner)

    def block_event_4():
        block_wait(across, q3)
        block_send(across, q3, row=partner)
        block_wait(across, q2)
        block_send(across, q2, row=partner)
        for q in range(ND):
            block_wait((partner + 4) % NR, q)

    def near_blocks():
        for b in (partner, (partner + 2) % NR, (partner + 6) % NR):
            for q in range(ND):
                block_wait(b, q)

    def chunk(source, lo, hi):
        left_op = zg[source, lo:hi]
        right_op = blk[source // 2, at(source % 2, width), :]
        acc[lo:hi] += product3(left_op, right_op, NN)

    def middle_chunks(ready, lo, hi):
        def one(i, _):
            source = (z + i + NC - 4) % NC

            @pl.when((source // 4 != across // 2) == ready)
            def _():
                chunk(source, 0, part)

            return 0

        lax.fori_loop(lo, hi, one, 0)

    def chunks(k, lo=0, hi=part):
        terms = []
        for source in ((z + k) % NC, (z + NC - k) % NC):
            terms.append(product3(zg[source, lo:hi], blk[source // 2, at(source % 2, width), :], NN))
        acc[lo:hi] += terms[0] + terms[1]

    ring(0, EARLY)
    for k in range(1, ND):
        go(remote(zall.at[r, d], zall.at[r, d], gsend.at[k], grecv_x.at[d], depth=(d + k) % ND))
    ring(0, LATE)
    for k in range(1, ND):
        q = (d + k) % ND
        arrived(zall.at[r, q], grecv_x.at[q])
    for k, peer in enumerate((above, below, across, partner)):
        go(remote(zall.at[r], zall.at[r], gsend.at[4 + k], grecv_r.at[r], row=peer))
    block_send(r, q0, row=above)
    block_send(r, q1, row=below)
    block_send(r, q1, row=above)
    block_send(r, q0, row=below)
    for q in range(ND):
        block_send(r, q, row=partner)

    ring(1, EARLY)
    tell(token_2, 2)
    ring(1, LATE)
    for k, peer in enumerate((above, below, across)):
        arrived(zall.at[peer], grecv_r.at[peer])
        go(remote(zall.at[peer], zall.at[peer], gsend.at[8 + k], grecv_r.at[peer], row=partner))
    ring(2, EARLY)
    pl.semaphore_wait(token_2, 2)
    tell(token_4, 4)

    for peer in (partner, (partner + 2) % NR, (partner + 4) % NR, (partner + 6) % NR):
        arrived(zall.at[peer], grecv_r.at[peer])
    rank = NR * zall.shape[2]
    factor = jnp.concatenate([zall[:, x].reshape(rank, zall.shape[3]) for x in range(ND)], axis=1)
    own = app.shape[0]
    for b in range(ND):
        partial = product3(blk[r, pl.ds(b * part, part), :], factor, NT)
        for i in range(part // own):
            value = partial[i * own : (i + 1) * own]
            pst[i % ND, i // ND, b, 0:own] = value[:, :LANES]
            pst[i % ND, i // ND, b, own : 2 * own] = value[:, LANES:]
    s_hi, s_lo = split(factor * factor)
    ones = jnp.ones((8, width), BF16)
    old = lax.dot_general(ones, s_hi, NT, preferred_element_type=F32) + lax.dot_general(
        ones, s_lo, NT, preferred_element_type=F32
    )
    sx[here, 2] = old[0, :LANES]
    sx[here, 3] = old[0, LANES:]
    two_up, two_down = (z + 2) % NC, (z + NC - 2) % NC
    low, high = pl.ds(0, 2), pl.ds(2, 2)
    go(remote(pst.at[d, up % 4], r1.at[0], psend.at[0], precv1.at[0], col=up))
    go(remote(pst.at[d, down % 4], r1.at[1], psend.at[1], precv1.at[1], col=down))
    go(remote(pst.at[d, two_down % 4, low], r1.at[2, low], psend.at[2], precv1.at[2], col=two_down))
    go(remote(pst.at[d, two_up % 4, high], r1.at[2, high], psend.at[6], precv1.at[3], col=two_up))

    ring(2, LATE)
    block_event_1()
    ring(3, EARLY)
    ring(3, LATE)
    block_event_2()
    arrived(r1.at[0], precv1.at[0])
    arrived(r1.at[1], precv1.at[1])
    arrived(r1.at[2, low], precv1.at[2])
    arrived(r1.at[2, high], precv1.at[3])
    s1[...] = (pst[d, pos] + r1[0]) + (r1[1] + r1[2])
    pl.semaphore_wait(token_4, 2)
    for k in range(1, 4):
        q = (grp + k) % 4
        go(remote(s1.at[q], r2.at[grp], psend.at[2 + k], precv2.at[grp], col=q * 4 + pos))
    ring(4, EARLY)
    drain(60)
    ring(4, LATE)
    block_event_3()
    ring(5, EARLY)
    near_blocks()
    middle_chunks(True, 3, 6)
    ring(5, LATE)
    new = s1[grp]
    for k in range(1, 4):
        q = (grp + k) % 4
        arrived(r2.at[q], precv2.at[q])
        new = new + r2[q]
    app[:, :LANES] = new[:own]
    app[:, LANES:] = new[own:]
    squares = new * new
    sx[here, 0] = jnp.sum(squares[:own], axis=0)
    sx[here, 1] = jnp.sum(squares[own:], axis=0)
    for k in range(1, NR * ND):
        peer = (here + k) % (NR * ND)
        go(remote(sx.at[here], sx.at[here], ssend.at[k], srecv_x.at[here], row=peer // ND, depth=peer % ND))
    middle_chunks(True, 1, 3)
    middle_chunks(True, 6, 8)
    ring(6, EARLY)
    block_event_4()
    middle_chunks(True, 0, 1)
    middle_chunks(True, 8, 9)
    middle_chunks(False, 0, 4)
    ring(6, LATE)
    for k in range(1, NR * ND):
        peer = (here + k) % (NR * ND)
        arrived(sx.at[peer], srecv_x.at[peer])
    sums = jnp.sum(sx[...], axis=0)
    plane[0] = sums[0:2]
    plane[1] = sums[2:4]
    sz[z] = plane[core]
    for k in range(1, NC):
        go(remote(sz.at[z], sz.at[z], ssend.at[NR * ND + k], srecv_z.at[z], col=(z + k) % NC))
    middle_chunks(False, 4, 9)
    drain(60)
    ring(7, EARLY)
    chunks(5)
    ring(7, LATE)
    chunks(6)
    chunks(7)
    ring(8, EARLY)
    chunk((z + 8) % NC, 0, first)

    wide = width // ND
    turned = acc[0:first].T
    for x in range(ND):
        stage_e[x] = turned[x * wide : (x + 1) * wide]
    for k in (2, 1, 3):
        q = (d + k) % ND
        go(remote(stage_e.at[q], cout_e.at[d], csend.at[k], crecv_e.at[d], depth=q))
    cout_e[d] = stage_e[d]
    ring(8, LATE)
    chunk((z + 8) % NC, first, part)
    turned = acc[first:part].T
    for x in range(ND):
        block = turned[x * wide : (x + 1) * wide]
        stage_l[x] = jnp.concatenate([block[: wide // 2], block[wide // 2 :]], axis=1)
    for k in (2, 1, 3):
        q = (d + k) % ND
        go(remote(stage_l.at[q], cout_l.at[d], csend.at[3 + k], crecv_l.at[d], depth=q))
    cout_l[d] = stage_l[d]

    for k in range(1, NC):
        q = (z + k) % NC
        arrived(sz.at[q], srecv_z.at[q])
    both[core] = jnp.sum(sz[...], axis=0)
    go(remote(both.at[core], both.at[core], ssend.at[0], srecv_c, row=partner))
    drain()
    arrived(both.at[1 - core], srecv_c)
    nrm[...] = jnp.sqrt(both[0]) / jnp.sqrt(both[1] * (1.0 / (NR * ND)) + 1e-06)
    for k in range(1, ND):
        q = (d + k) % ND
        arrived(cout_e.at[q], crecv_e.at[q])
        arrived(cout_l.at[q], crecv_l.at[q])


def finish(early, late, app_in, nrm_in, sq, app, nrm):
    half = early.shape[1] // 2
    app[...] = app_in[...]
    nrm[...] = nrm_in[...]
    for i in range(0, ND, 2):
        e0, e1 = early[i], early[i + 1]
        l0, l1 = late[i], late[i + 1]
        base = i * 3 * LANES // 2
        sq[:, base : base + LANES] = e0
        l0_cols = jnp.concatenate([l0[:, :64], l0[:, 64:]], axis=0)
        l1_cols = jnp.concatenate([l1[:, :64], l1[:, 64:]], axis=0)
        sq[:, base + LANES : base + 2 * LANES] = jnp.concatenate([l0_cols, e1[:, :64]], axis=1)
        sq[:, base + 2 * LANES : base + 3 * LANES] = jnp.concatenate([e1[:, 64:], l1_cols], axis=1)


def body(state_matrix, gram_factor):
    rows, width = state_matrix.shape
    factor_rows, factor_cols = gram_factor.shape
    part = rows // ND
    rank = factor_cols * NR
    wide = width // ND
    own = rows // (NC * ND)
    dma = pltpu.SemaphoreType.DMA
    vmem = lambda *shape: pltpu.VMEM(shape, F32)
    shape = lambda *dims: jax.ShapeDtypeStruct(dims, F32)
    whole = pl.BlockSpec(memory_space=pltpu.VMEM)
    parts = pl.pallas_call(
        kernel,
        out_shape=(shape(ND, wide, LANES), shape(ND, wide // 2, LANES), shape(own, rank), shape(2, LANES)),
        in_specs=[pl.BlockSpec(memory_space=pltpu.HBM)] * 2,
        out_specs=[whole] * 4,
        scratch_shapes=[
            vmem(NC, part, width),
            vmem(NR, rows, width),
            vmem(NR, ND, factor_cols, factor_rows),
            vmem(ND, 4, 4, 2 * own, LANES),
            vmem(3, 4, 2 * own, LANES),
            vmem(4, 2 * own, LANES),
            vmem(4, 2 * own, LANES),
            vmem(NR * ND, 4, LANES),
            vmem(2, 2, LANES),
            vmem(NC, 2, LANES),
            vmem(2, 2, LANES),
            vmem(part, width),
            vmem(ND, wide, LANES),
            vmem(ND, wide // 2, LANES),
            dma((3,)),
            dma((2, 8, SUBS)),
            dma((2, 8, SUBS)),
            dma((40,)),
            dma((NR, ND)),
            dma((12,)),
            dma((ND,)),
            dma((NR,)),
            dma((8,)),
            dma((4,)),
            dma((4,)),
            dma((NR * ND + NC,)),
            dma((NR * ND,)),
            dma((NC,)),
            dma,
            dma((8,)),
            dma((ND,)),
            dma((ND,)),
            pltpu.SemaphoreType.REGULAR,
            pltpu.SemaphoreType.REGULAR,
        ],
        compiler_params=pltpu.CompilerParams(
            collective_id=0, has_side_effects=True, vmem_limit_bytes=55900000
        ),
    )(state_matrix, gram_factor.T)
    squared, appended, norm = pl.pallas_call(
        finish,
        out_shape=(shape(wide, rows), shape(own, rank), shape(2, LANES)),
        in_specs=[whole] * 4,
        out_specs=[whole] * 3,
        compiler_params=pltpu.CompilerParams(vmem_limit_bytes=8 * 1024 * 1024),
    )(*parts)
    return squared.T, appended, norm.reshape(rank)


def solution(mesh):
    in_specs = (P("row", "col"), P(("col", "depth"), "row"))
    out_specs = (P("row", ("col", "depth")), P(("row", "col", "depth"), None), P())
    return jax.shard_map(body, mesh=mesh, in_specs=in_specs, out_specs=out_specs, check_vma=False)
```

```python
import functools

import jax
import jax.numpy as jnp
from jax import lax
from jax.experimental import pallas as pl
from jax.experimental.pallas import tpu as pltpu
from jax.sharding import PartitionSpec as P

MESH = pl.DeviceIdType.MESH
NR, NC, ND = 8, 16, 4
SUBS = 6
EARLY = range(4)
LATE = range(4, 6)
LANES = 128
F32 = jnp.float32
BF16 = jnp.bfloat16
NT = (((1,), (1,)), ((), ()))
NN = (((1,), (0,)), ((), ()))


def split(v):
    hi = v.astype(BF16)
    return hi, (v - hi.astype(F32)).astype(BF16)


def product3(a, b, dims):
    a_hi, a_lo = split(a)
    b_hi, b_lo = split(b)
    dot = functools.partial(lax.dot_general, dimension_numbers=dims, preferred_element_type=F32)
    return dot(a_hi, b_hi) + (dot(a_hi, b_lo) + dot(a_lo, b_hi))


def kernel(
    a_hbm, g_hbm, cout_e, cout_l, app, nrm,
    zg, blk, zall, pst, r1, s1, r2, sx, plane, sz, both, acc, stage_e, stage_l,
    lsem, zsend, zrecv, bsend, brecv, gsend, grecv_x, grecv_r, psend, precv1, precv2,
    ssend, srecv_x, srecv_z, srecv_c, csend, crecv_e, crecv_l, token_2, token_4,
):
    r, z, d = lax.axis_index("row"), lax.axis_index("col"), lax.axis_index("depth")
    rows, width = blk.shape[1], blk.shape[2]
    part = rows // ND
    sub = part // SUBS
    first = sub * len(EARLY)
    core = r % 2
    partner = r + 1 - 2 * core
    pos, grp = z % 4, z // 4
    here = r * ND + d
    up, down = (z + 1) % NC, (z + NC - 1) % NC
    above, below, across = (r + 2) % NR, (r + NR - 2) % NR, (r + 4) % NR
    right, left = (d + 1) % ND, (d + ND - 1) % ND

    def at(i, size):
        return pl.ds(pl.multiple_of(i * size, 8), size)

    def remote(src, dst, send, recv, **device):
        return pltpu.make_async_remote_copy(
            src_ref=src, dst_ref=dst, send_sem=send, recv_sem=recv, device_id=device, device_id_type=MESH
        )

    started = []

    def go(copy):
        copy.start()
        started.append(copy)

    def drain(left=0):
        while len(started) > left:
            started.pop(0).wait_send()

    def tell(token, distance):
        for peer in ((z + distance) % NC, (z + NC - distance) % NC):
            pl.semaphore_signal(token, inc=1, device_id={"col": peer}, device_id_type=MESH)

    def arrived(ref, recv):
        remote(ref, ref, csend.at[0], recv, row=partner).wait_recv()

    load_own = pltpu.make_async_copy(a_hbm.at[at(d, part), :], zg.at[z], lsem.at[0])
    load_gram = pltpu.make_async_copy(g_hbm, zall.at[r, d], lsem.at[1])
    load_block = pltpu.make_async_copy(a_hbm, blk.at[r], lsem.at[2])
    load_own.start()
    load_gram.start()
    load_block.start()

    barrier = pltpu.get_barrier_semaphore()
    peers = [{"col": up}, {"col": down}]
    peers += [{"depth": (d + k) % ND} for k in range(1, ND)]
    peers += [{"row": above}, {"row": below}, {"row": across}, {"row": partner}]
    for peer in peers:
        pl.semaphore_signal(barrier, inc=1, device_id=peer, device_id_type=MESH)
    acc[...] = jnp.zeros_like(acc)
    load_own.wait()
    load_gram.wait()
    load_block.wait()
    pl.semaphore_wait(barrier, len(peers))

    def piece(way, k, s):
        source = (z - k + NC) % NC if way == 0 else (z + k) % NC
        return zg.at[source, pl.ds(s * sub, sub), :]

    def travels(way, k, s):
        return k < 7 or s % 2 == way

    def ring(k, subs):
        for s in subs:
            for way in (0, 1):
                if k > 0 and travels(way, k - 1, s):
                    arrived(piece(way, k, s), zrecv.at[way, k - 1, s])
                if k < 8 and travels(way, k, s):
                    ref = piece(way, k, s)
                    go(remote(ref, ref, zsend.at[way, k, s], zrecv.at[way, k, s], col=up if way == 0 else down))

    n_sent = [0]

    def block_piece(b, q):
        return blk.at[b, at(q, part), :]

    def block_send(b, q, **device):
        go(remote(block_piece(b, q), block_piece(b, q), bsend.at[n_sent[0]], brecv.at[b, q], **device))
        n_sent[0] += 1

    def block_wait(b, q):
        arrived(block_piece(b, q), brecv.at[b, q])

    q0, q1, q2, q3 = d, (d + 1) % ND, (d + 2) % ND, (d + 3) % ND

    def block_event_1():
        block_wait(below, q0)
        block_send(below, q0, row=above)
        block_send(below, q0, depth=right)
        block_send(below, q0, row=partner)
        block_wait(above, q1)
        block_send(above, q1, row=below)
        block_send(above, q1, depth=left)
        block_send(above, q1, row=partner)

    def block_event_2():
        block_wait(below, q1)
        block_send(below, q1, depth=left)
        block_send(below, q1, row=partner)
        block_wait(above, q0)
        block_send(above, q0, depth=right)
        block_send(above, q0, row=partner)
        block_wait(below, q3)
        block_send(below, q3, row=partner)
        block_wait(above, q2)
        block_send(above, q2, row=partner)

    def block_event_3():
        block_wait(across, q0)
        block_send(across, q0, depth=right)
        block_send(across, q0, row=partner)
        block_wait(across, q1)
        block_send(across, q1, depth=left)
        block_send(across, q1, row=partner)
        block_wait(above, q3)
        block_send(above, q3, row=partner)
        block_wait(below, q2)
        block_send(below, q2, row=partner)

    def block_event_4():
        block_wait(across, q3)
        block_send(across, q3, row=partner)
        block_wait(across, q2)
        block_send(across, q2, row=partner)
        for q in range(ND):
            block_wait((partner + 4) % NR, q)

    def near_blocks():
        for b in (partner, (partner + 2) % NR, (partner + 6) % NR):
            for q in range(ND):
                block_wait(b, q)

    def chunk(source, lo, hi):
        left_op = zg[source, lo:hi]
        right_op = blk[source // 2, at(source % 2, width), :]
        acc[lo:hi] += product3(left_op, right_op, NN)

    def middle_chunks(ready, lo, hi):
        def one(i, _):
            source = (z + i + NC - 4) % NC

            @pl.when((source // 4 != across // 2) == ready)
            def _():
                chunk(source, 0, part)

            return 0

        lax.fori_loop(lo, hi, one, 0)

    def chunks(k, lo=0, hi=part):
        terms = []
        for source in ((z + k) % NC, (z + NC - k) % NC):
            terms.append(product3(zg[source, lo:hi], blk[source // 2, at(source % 2, width), :], NN))
        acc[lo:hi] += terms[0] + terms[1]

    ring(0, EARLY)
    for k in range(1, ND):
        go(remote(zall.at[r, d], zall.at[r, d], gsend.at[k], grecv_x.at[d], depth=(d + k) % ND))
    ring(0, LATE)
    for k in range(1, ND):
        q = (d + k) % ND
        arrived(zall.at[r, q], grecv_x.at[q])
    for k, peer in enumerate((above, below, across, partner)):
        go(remote(zall.at[r], zall.at[r], gsend.at[4 + k], grecv_r.at[r], row=peer))
    block_send(r, q0, row=above)
    block_send(r, q1, row=below)
    block_send(r, q1, row=above)
    block_send(r, q0, row=below)
    for q in range(ND):
        block_send(r, q, row=partner)

    ring(1, EARLY)
    tell(token_2, 2)
    ring(1, LATE)
    for k, peer in enumerate((above, below, across)):
        arrived(zall.at[peer], grecv_r.at[peer])
        go(remote(zall.at[peer], zall.at[peer], gsend.at[8 + k], grecv_r.at[peer], row=partner))
    ring(2, EARLY)
    pl.semaphore_wait(token_2, 2)
    tell(token_4, 4)

    for peer in (partner, (partner + 2) % NR, (partner + 4) % NR, (partner + 6) % NR):
        arrived(zall.at[peer], grecv_r.at[peer])
    rank = NR * zall.shape[2]
    factor = jnp.concatenate([zall[:, x].reshape(rank, zall.shape[3]) for x in range(ND)], axis=1)
    own = app.shape[0]
    for b in range(ND):
        partial = product3(blk[r, pl.ds(b * part, part), :], factor, NT)
        for i in range(part // own):
            value = partial[i * own : (i + 1) * own]
            pst[i % ND, i // ND, b, 0:own] = value[:, :LANES]
            pst[i % ND, i // ND, b, own : 2 * own] = value[:, LANES:]
    s_hi, s_lo = split(factor * factor)
    ones = jnp.ones((8, width), BF16)
    old = lax.dot_general(ones, s_hi, NT, preferred_element_type=F32) + lax.dot_general(
        ones, s_lo, NT, preferred_element_type=F32
    )
    sx[here, 2] = old[0, :LANES]
    sx[here, 3] = old[0, LANES:]
    two_up, two_down = (z + 2) % NC, (z + NC - 2) % NC
    low, high = pl.ds(0, 2), pl.ds(2, 2)
    go(remote(pst.at[d, up % 4], r1.at[0], psend.at[0], precv1.at[0], col=up))
    go(remote(pst.at[d, down % 4], r1.at[1], psend.at[1], precv1.at[1], col=down))
    go(remote(pst.at[d, two_down % 4, low], r1.at[2, low], psend.at[2], precv1.at[2], col=two_down))
    go(remote(pst.at[d, two_up % 4, high], r1.at[2, high], psend.at[6], precv1.at[3], col=two_up))

    ring(2, LATE)
    block_event_1()
    ring(3, EARLY)
    ring(3, LATE)
    block_event_2()
    arrived(r1.at[0], precv1.at[0])
    arrived(r1.at[1], precv1.at[1])
    arrived(r1.at[2, low], precv1.at[2])
    arrived(r1.at[2, high], precv1.at[3])
    s1[...] = (pst[d, pos] + r1[0]) + (r1[1] + r1[2])
    pl.semaphore_wait(token_4, 2)
    for k in range(1, 4):
        q = (grp + k) % 4
        go(remote(s1.at[q], r2.at[grp], psend.at[2 + k], precv2.at[grp], col=q * 4 + pos))
    ring(4, EARLY)
    drain(60)
    ring(4, LATE)
    block_event_3()
    ring(5, EARLY)
    new = s1[grp]
    for k in range(1, 4):
        q = (grp + k) % 4
        arrived(r2.at[q], precv2.at[q])
        new = new + r2[q]
    app[:, :LANES] = new[:own]
    app[:, LANES:] = new[own:]
    squares = new * new
    sx[here, 0] = jnp.sum(squares[:own], axis=0)
    sx[here, 1] = jnp.sum(squares[own:], axis=0)
    for k in range(1, NR * ND):
        peer = (here + k) % (NR * ND)
        go(remote(sx.at[here], sx.at[here], ssend.at[k], srecv_x.at[here], row=peer // ND, depth=peer % ND))
    near_blocks()
    middle_chunks(True, 3, 6)
    ring(5, LATE)
    middle_chunks(True, 1, 3)
    middle_chunks(True, 6, 8)
    ring(6, EARLY)
    block_event_4()
    for k in range(1, NR * ND):
        peer = (here + k) % (NR * ND)
        arrived(sx.at[peer], srecv_x.at[peer])
    sums = jnp.sum(sx[...], axis=0)
    plane[0] = sums[0:2]
    plane[1] = sums[2:4]
    sz[z] = plane[core]
    for k in range(1, NC):
        go(remote(sz.at[z], sz.at[z], ssend.at[NR * ND + k], srecv_z.at[z], col=(z + k) % NC))
    middle_chunks(True, 0, 1)
    middle_chunks(True, 8, 9)
    middle_chunks(False, 0, 4)
    ring(6, LATE)
    middle_chunks(False, 4, 9)
    drain(60)
    ring(7, EARLY)
    chunks(5)
    ring(7, LATE)
    chunks(6)
    chunks(7)
    ring(8, EARLY)
    chunk((z + 8) % NC, 0, first)

    wide = width // ND
    turned = acc[0:first].T
    for x in range(ND):
        stage_e[x] = turned[x * wide : (x + 1) * wide]
    for k in (2, 1, 3):
        q = (d + k) % ND
        go(remote(stage_e.at[q], cout_e.at[d], csend.at[k], crecv_e.at[d], depth=q))
    cout_e[d] = stage_e[d]
    ring(8, LATE)
    chunk((z + 8) % NC, first, part)
    turned = acc[first:part].T
    for x in range(ND):
        block = turned[x * wide : (x + 1) * wide]
        stage_l[x] = jnp.concatenate([block[: wide // 2], block[wide // 2 :]], axis=1)
    for k in (2, 1, 3):
        q = (d + k) % ND
        go(remote(stage_l.at[q], cout_l.at[d], csend.at[3 + k], crecv_l.at[d], depth=q))
    cout_l[d] = stage_l[d]

    for k in range(1, NC):
        q = (z + k) % NC
        arrived(sz.at[q], srecv_z.at[q])
    both[core] = jnp.sum(sz[...], axis=0)
    go(remote(both.at[core], both.at[core], ssend.at[0], srecv_c, row=partner))
    drain()
    arrived(both.at[1 - core], srecv_c)
    nrm[...] = jnp.sqrt(both[0]) / jnp.sqrt(both[1] * (1.0 / (NR * ND)) + 1e-06)
    for k in range(1, ND):
        q = (d + k) % ND
        arrived(cout_e.at[q], crecv_e.at[q])
        arrived(cout_l.at[q], crecv_l.at[q])


def finish(early, late, app_in, nrm_in, sq, app, nrm):
    half = early.shape[1] // 2
    app[...] = app_in[...]
    nrm[...] = nrm_in[...]
    for i in range(0, ND, 2):
        e0, e1 = early[i], early[i + 1]
        l0, l1 = late[i], late[i + 1]
        base = i * 3 * LANES // 2
        sq[:, base : base + LANES] = e0
        l0_cols = jnp.concatenate([l0[:, :64], l0[:, 64:]], axis=0)
        l1_cols = jnp.concatenate([l1[:, :64], l1[:, 64:]], axis=0)
        sq[:, base + LANES : base + 2 * LANES] = jnp.concatenate([l0_cols, e1[:, :64]], axis=1)
        sq[:, base + 2 * LANES : base + 3 * LANES] = jnp.concatenate([e1[:, 64:], l1_cols], axis=1)


def body(state_matrix, gram_factor):
    rows, width = state_matrix.shape
    factor_rows, factor_cols = gram_factor.shape
    part = rows // ND
    rank = factor_cols * NR
    wide = width // ND
    own = rows // (NC * ND)
    dma = pltpu.SemaphoreType.DMA
    vmem = lambda *shape: pltpu.VMEM(shape, F32)
    shape = lambda *dims: jax.ShapeDtypeStruct(dims, F32)
    whole = pl.BlockSpec(memory_space=pltpu.VMEM)
    parts = pl.pallas_call(
        kernel,
        out_shape=(shape(ND, wide, LANES), shape(ND, wide // 2, LANES), shape(own, rank), shape(2, LANES)),
        in_specs=[pl.BlockSpec(memory_space=pltpu.HBM)] * 2,
        out_specs=[whole] * 4,
        scratch_shapes=[
            vmem(NC, part, width),
            vmem(NR, rows, width),
            vmem(NR, ND, factor_cols, factor_rows),
            vmem(ND, 4, 4, 2 * own, LANES),
            vmem(3, 4, 2 * own, LANES),
            vmem(4, 2 * own, LANES),
            vmem(4, 2 * own, LANES),
            vmem(NR * ND, 4, LANES),
            vmem(2, 2, LANES),
            vmem(NC, 2, LANES),
            vmem(2, 2, LANES),
            vmem(part, width),
            vmem(ND, wide, LANES),
            vmem(ND, wide // 2, LANES),
            dma((3,)),
            dma((2, 8, SUBS)),
            dma((2, 8, SUBS)),
            dma((40,)),
            dma((NR, ND)),
            dma((12,)),
            dma((ND,)),
            dma((NR,)),
            dma((8,)),
            dma((4,)),
            dma((4,)),
            dma((NR * ND + NC,)),
            dma((NR * ND,)),
            dma((NC,)),
            dma,
            dma((8,)),
            dma((ND,)),
            dma((ND,)),
            pltpu.SemaphoreType.REGULAR,
            pltpu.SemaphoreType.REGULAR,
        ],
        compiler_params=pltpu.CompilerParams(
            collective_id=0, has_side_effects=True, vmem_limit_bytes=55900000
        ),
    )(state_matrix, gram_factor.T)
    squared, appended, norm = pl.pallas_call(
        finish,
        out_shape=(shape(wide, rows), shape(own, rank), shape(2, LANES)),
        in_specs=[whole] * 4,
        out_specs=[whole] * 3,
        compiler_params=pltpu.CompilerParams(vmem_limit_bytes=8 * 1024 * 1024),
    )(*parts)
    return squared.T, appended, norm.reshape(rank)


def solution(mesh):
    in_specs = (P("row", "col"), P(("col", "depth"), "row"))
    out_specs = (P("row", ("col", "depth")), P(("row", "col", "depth"), None), P())
    return jax.shard_map(body, mesh=mesh, in_specs=in_specs, out_specs=out_specs, check_vma=False)
```
